32 devices in a mesh: dp: 4 (over y, z), sp: 8 (over x, core).
Axes of the slice: x: 4, y: 2, z: 2, core: 2. Of those that a mesh axis runs over, the one named last changes fastest.
The devices are a block of a 4x4x8 slice.
Arguments:
- tokens: bfloat16 [131072, 1024], P(('dp', 'sp')), parts along dimension 0
- w_q: bfloat16 [1024, 1024], replicated
- w_k: bfloat16 [1024, 1024], replicated
- w_v: bfloat16 [1024, 1024], replicated
- w_o: bfloat16 [1024, 1024], replicated
- grad_y: bfloat16 [131072, 1024], P(('dp', 'sp')), parts along dimension 0
Outputs:
- output 1: bfloat16 [131072, 1024], P(('dp', 'sp')), parts along dimension 0
- output 2: bfloat16 [131072, 1024], P(('dp', 'sp')), parts along dimension 0
- output 3: float32 [4096, 1024], P('dp'), parts along dimension 0
- output 4: float32 [4096, 1024], P('dp'), parts along dimension 0
- output 5: float32 [4096, 1024], P('dp'), parts along dimension 0
- output 6: float32 [4096, 1024], P('dp'), parts along dimension 0
There are 4 independent parts. The reference program is written for one: setup_inputs(seed, part) draws one part's arguments, and reference() takes and returns one part's arrays. A program takes and returns all parts, laid end to end along the dimension named above; an argument that names none is the same for every part.
All inputs are finite; a program needn't handle non-finite values.
Results may differ from the reference program's by a relative error of at most 0.00401916.
Values are sent between devices in bfloat16 or wider.
A program may use at most 768 MiB of HBM per device.

```python
import math
import jax
import jax.numpy as jnp

SEQ_LEN = 32768
MODEL_DIM = 1024
HEAD_DIM = 128
BLOCK_LEN = 128


def setup_inputs(seed: int = 0, part: int = 0) -> dict:
    part_key = jax.random.fold_in(jax.random.key(seed), part)
    key_x, key_dy = jax.random.split(part_key)
    key_q, key_k, key_v, key_o = jax.random.split(jax.random.key(seed + 1), 4)
    w_scale = MODEL_DIM ** -0.5
    shape_w = (MODEL_DIM, MODEL_DIM)

    def normal_weight(key_w):
        return (jax.random.normal(key_w, shape_w, jnp.float32) * w_scale).astype(jnp.bfloat16)

    tokens = jax.random.normal(key_x, (SEQ_LEN, MODEL_DIM), jnp.float32)
    grad_y = jax.random.normal(key_dy, (SEQ_LEN, MODEL_DIM), jnp.float32) * SEQ_LEN ** -0.25
    return {"tokens": tokens.astype(jnp.bfloat16), "w_q": normal_weight(key_q), "w_k": normal_weight(key_k), "w_v": normal_weight(key_v), "w_o": normal_weight(key_o), "grad_y": grad_y.astype(jnp.bfloat16)}


def reference(tokens, w_q, w_k, w_v, w_o, grad_y):
    n_heads = MODEL_DIM // HEAD_DIM
    n_blocks = SEQ_LEN // BLOCK_LEN
    att_scale = 1.0 / math.sqrt(SEQ_LEN * HEAD_DIM)
    causal = jnp.arange(BLOCK_LEN)[:, None] >= jnp.arange(BLOCK_LEN)[None, :]

    def project(operand, weight):
        return jnp.dot(operand, weight, preferred_element_type=jnp.float32).astype(jnp.bfloat16)

    def split_heads(tensor):
        return tensor.reshape(n_blocks, BLOCK_LEN, n_heads, HEAD_DIM).astype(jnp.float32)

    def to_rows(tensor):
        return (tensor * att_scale).astype(jnp.bfloat16).reshape(SEQ_LEN, MODEL_DIM)

    def as_bf16(tensor):
        return tensor.astype(jnp.bfloat16).astype(jnp.float32)

    def excl_prefix(blocks):
        zero_block = jnp.zeros_like(blocks[:1])
        return jnp.concatenate([zero_block, jnp.cumsum(blocks, axis=0)[:-1]], axis=0)

    q_heads = split_heads(project(tokens, w_q))
    k_heads = split_heads(project(tokens, w_k))
    v_heads = split_heads(project(tokens, w_v))
    fwd_state = as_bf16(excl_prefix(jnp.einsum("nshd,nshe->nhde", k_heads, v_heads)))
    masked_scores = as_bf16(jnp.where(causal, jnp.einsum("nthd,nshd->nhts", q_heads, k_heads), 0.0))
    out_rows = to_rows(jnp.einsum("nhts,nshe->nthe", masked_scores, v_heads) + jnp.einsum("nthd,nhde->nthe", q_heads, fwd_state))
    out_y = project(out_rows, w_o)

    do_heads = split_heads(project(grad_y, w_o.T))
    block_qdo = jnp.einsum("nthd,nthe->nhde", q_heads, do_heads)
    rev_state = as_bf16(excl_prefix(block_qdo[::-1])[::-1])
    masked_grads = as_bf16(jnp.where(causal, jnp.einsum("nthe,nshe->nhts", do_heads, v_heads), 0.0))
    dq_rows = to_rows(jnp.einsum("nhts,nshd->nthd", masked_grads, k_heads) + jnp.einsum("nthe,nhde->nthd", do_heads, fwd_state))
    dk_rows = to_rows(jnp.einsum("nhts,nthd->nshd", masked_grads, q_heads) + jnp.einsum("nshe,nhde->nshd", v_heads, rev_state))
    dv_rows = to_rows(jnp.einsum("nhts,nthe->nshe", masked_scores, do_heads) + jnp.einsum("nshd,nhde->nshe", k_heads, rev_state))
    grad_x = (jnp.dot(dq_rows, w_q.T, preferred_element_type=jnp.float32) + jnp.dot(dk_rows, w_k.T, preferred_element_type=jnp.float32) + jnp.dot(dv_rows, w_v.T, preferred_element_type=jnp.float32)).astype(jnp.bfloat16)
    grad_wq = jnp.dot(tokens.T, dq_rows, preferred_element_type=jnp.float32)
    grad_wk = jnp.dot(tokens.T, dk_rows, preferred_element_type=jnp.float32)
    grad_wv = jnp.dot(tokens.T, dv_rows, preferred_element_type=jnp.float32)
    grad_wo = jnp.dot(out_rows.T, grad_y, preferred_element_type=jnp.float32)
    return (out_y, grad_x, grad_wq, grad_wk, grad_wv, grad_wo)
```

```python
import functools
import math
import jax
import jax.numpy as jnp
from jax import lax
from jax.experimental import pallas as pl
from jax.experimental.pallas import tpu as pltpu
from jax.sharding import PartitionSpec as P

HEAD_DIM = 128
BLOCK_LEN = 128
BF16 = jnp.bfloat16
F32 = jnp.float32
MESH = pl.DeviceIdType.MESH
VMEM_LIMIT = 64 * 1024 * 1024 - 1024 * 64


def dot(a, b):
    return lax.dot_general(a, b, (((1,), (0,)), ((), ())), preferred_element_type=F32)


def dot_nt(a, b):
    return lax.dot_general(a, b, (((1,), (1,)), ((), ())), preferred_element_type=F32)


def dot_tn(a, b):
    return lax.dot_general(a, b, (((0,), (0,)), ((), ())), preferred_element_type=F32)


def project_kernel(x_ref, dy_ref, wq_ref, wk_ref, wv_ref, wo_ref, q_ref, k_ref, v_ref, do_ref, tot_ref):
    @pl.when(pl.program_id(0) == 0)
    def _():
        tot_ref[...] = jnp.zeros_like(tot_ref)

    x = x_ref[...]
    q_ref[...] = dot(x, wq_ref[...]).astype(BF16)
    k_ref[...] = dot(x, wk_ref[...]).astype(BF16)
    v_ref[...] = dot(x, wv_ref[...]).astype(BF16)
    do_ref[...] = dot_nt(dy_ref[...], wo_ref[...]).astype(BF16)
    n_heads = x.shape[1] // HEAD_DIM
    for h in range(n_heads):
        cols = slice(h * HEAD_DIM, (h + 1) * HEAD_DIM)
        tot_ref[0, h] += dot_tn(k_ref[:, cols], v_ref[:, cols])
        tot_ref[1, h] += dot_tn(q_ref[:, cols], do_ref[:, cols])


def exchange_kernel(n_chips, tot_ref, init_ref, part, chip, recv, half, d2d_sem, send_sem, recv_sem, half_sem):
    me = lax.axis_index("sp")
    my_chip, core = me // 2, me % 2
    partner = my_chip * 2 + (1 - core)
    n_heads = tot_ref.shape[1]
    n_half = n_heads // 2
    barrier = pltpu.get_barrier_semaphore()
    peers = [partner] + [((my_chip + o) % n_chips) * 2 + core for o in range(1, n_chips)]
    for peer in peers:
        pl.semaphore_signal(barrier, inc=1, device_id={"sp": peer}, device_id_type=MESH)
    pl.semaphore_wait(barrier, len(peers))

    first = pltpu.make_async_remote_copy(tot_ref, part, d2d_sem.at[0], d2d_sem.at[1], device_id={"sp": partner}, device_id_type=MESH)
    first.start()
    first.wait()
    mine = pl.ds(core * n_half, n_half)
    chip[...] = tot_ref[:, mine] + part[:, mine]
    copies = []
    for o in range(1, n_chips):
        target = (my_chip + o) % n_chips
        kind = jnp.where(target > my_chip, 0, 1)
        copy = pltpu.make_async_remote_copy(chip.at[kind], recv.at[o - 1], send_sem.at[o - 1], recv_sem.at[o - 1],
                                            device_id={"sp": target * 2 + core}, device_id_type=MESH)
        copy.start()
        copies.append(copy)
    fwd = jnp.zeros_like(recv[0])
    rev = jnp.zeros_like(recv[0])
    for o in range(1, n_chips):
        copies[o - 1].wait()
        source = (my_chip + n_chips - o) % n_chips
        early = (source < my_chip).astype(F32)
        fwd = fwd + early * recv[o - 1]
        rev = rev + (1.0 - early) * recv[o - 1]
    half[0, 0] = fwd
    half[0, 1] = rev
    last = pltpu.make_async_remote_copy(half.at[0], half.at[1], half_sem.at[0], half_sem.at[1], device_id={"sp": partner}, device_id_type=MESH)
    last.start()
    last.wait()
    other = pl.ds((1 - core) * n_half, n_half)
    is_second = core.astype(F32)
    for slot, rows in ((0, mine), (1, other)):
        init_ref[0, rows] = half[slot, 0] + is_second * part[0, rows]
        init_ref[1, rows] = half[slot, 1] + (1.0 - is_second) * part[1, rows] + tot_ref[1, rows]


def attention_kernel(att_scale, q_ref, k_ref, v_ref, do_ref, init_ref, o_ref, dq_ref, dk_ref, dv_ref, state):
    @pl.when(pl.program_id(1) == 0)
    def _():
        state[...] = init_ref[...]

    n_rows, width = q_ref.shape
    row_id = lax.broadcasted_iota(jnp.int32, (BLOCK_LEN, BLOCK_LEN), 0)
    col_id = lax.broadcasted_iota(jnp.int32, (BLOCK_LEN, BLOCK_LEN), 1)
    causal = row_id >= col_id
    for h in range(width // HEAD_DIM):
        cols = slice(h * HEAD_DIM, (h + 1) * HEAD_DIM)
        s_run = state[0, h]
        r_run = state[1, h]
        for b in range(n_rows // BLOCK_LEN):
            rows = slice(b * BLOCK_LEN, (b + 1) * BLOCK_LEN)
            q, k, v, do = q_ref[rows, cols], k_ref[rows, cols], v_ref[rows, cols], do_ref[rows, cols]
            r_run = r_run - dot_tn(q, do)
            s16, r16 = s_run.astype(BF16), r_run.astype(BF16)
            a = jnp.where(causal, dot_nt(q, k), 0.0).astype(BF16)
            g = jnp.where(causal, dot_nt(do, v), 0.0).astype(BF16)
            o_ref[rows, cols] = (att_scale * (dot(a, v) + dot(q, s16))).astype(BF16)
            dq_ref[rows, cols] = (att_scale * (dot(g, k) + dot_nt(do, s16))).astype(BF16)
            dk_ref[rows, cols] = (att_scale * (dot_tn(g, q) + dot_nt(v, r16))).astype(BF16)
            dv_ref[rows, cols] = (att_scale * (dot_tn(a, do) + dot(k, r16))).astype(BF16)
            s_run = s_run + dot_tn(k, v)
        state[0, h] = s_run
        state[1, h] = r_run


def solution(mesh):
    n_seq = mesh.shape["sp"]
    row_spec = P(("dp", "sp"), None)
    grad_spec = P("dp", None)

    def local_layer(tokens, w_q, w_k, w_v, w_o, grad_y):
        n_rows, dim = tokens.shape
        n_heads = dim // HEAD_DIM
        att_scale = 1.0 / math.sqrt(n_rows * n_seq * HEAD_DIM)
        tile = 512
        rows_bf16 = jax.ShapeDtypeStruct((n_rows, dim), BF16)
        row_tile = pl.BlockSpec((tile, dim), lambda i: (i, 0))
        whole_w = pl.BlockSpec((dim, dim), lambda i: (0, 0), pipeline_mode=pl.Buffered(1))
        state_shape = (2, n_heads, HEAD_DIM, HEAD_DIM)
        q, k, v, do, totals = pl.pallas_call(
            project_kernel,
            grid=(n_rows // tile,),
            in_specs=[row_tile, row_tile] + [whole_w] * 4,
            out_specs=[row_tile] * 4 + [pl.BlockSpec(state_shape, lambda i: (0, 0, 0, 0))],
            out_shape=[rows_bf16] * 4 + [jax.ShapeDtypeStruct(state_shape, F32)],
            compiler_params=pltpu.CompilerParams(vmem_limit_bytes=VMEM_LIMIT, dimension_semantics=("arbitrary",)),
            name="project",
        )(tokens, grad_y, w_q, w_k, w_v, w_o)

        n_chips = n_seq // 2
        half_shape = (n_heads // 2, HEAD_DIM, HEAD_DIM)
        vmem = pl.BlockSpec(memory_space=pltpu.VMEM)
        init = pl.pallas_call(
            functools.partial(exchange_kernel, n_chips),
            in_specs=[vmem],
            out_specs=vmem,
            out_shape=jax.ShapeDtypeStruct(state_shape, F32),
            scratch_shapes=[
                pltpu.VMEM(state_shape, F32),
                pltpu.VMEM((2,) + half_shape, F32),
                pltpu.VMEM((n_chips - 1,) + half_shape, F32),
                pltpu.VMEM((2, 2) + half_shape, F32),
                pltpu.SemaphoreType.DMA((2,)),
                pltpu.SemaphoreType.DMA((n_chips - 1,)),
                pltpu.SemaphoreType.DMA((n_chips - 1,)),
                pltpu.SemaphoreType.DMA((2,)),
            ],
            compiler_params=pltpu.CompilerParams(vmem_limit_bytes=32 * 1024 * 1024, collective_id=0, has_side_effects=True),
            name="exchange",
        )(totals)

        width, chunk = 2 * HEAD_DIM, 512
        col_tile = pl.BlockSpec((chunk, width), lambda g, i: (i, g))
        o, dq, dk, dv = pl.pallas_call(
            functools.partial(attention_kernel, att_scale),
            grid=(dim // width, n_rows // chunk),
            in_specs=[col_tile] * 4 + [pl.BlockSpec((2, width // HEAD_DIM, HEAD_DIM, HEAD_DIM), lambda g, i: (0, g, 0, 0))],
            out_specs=[col_tile] * 4,
            out_shape=[rows_bf16] * 4,
            scratch_shapes=[pltpu.VMEM((2, width // HEAD_DIM, HEAD_DIM, HEAD_DIM), F32)],
            compiler_params=pltpu.CompilerParams(vmem_limit_bytes=32 * 1024 * 1024, dimension_semantics=("arbitrary", "arbitrary")),
            name="attention",
        )(q, k, v, do, init)

        def weight_grad(left, right):
            return jnp.einsum("nd,ne->de", left, right, preferred_element_type=F32)

        def back_proj(rows, weight):
            return jnp.einsum("ne,de->nd", rows, weight, preferred_element_type=F32)

        grads = lax.psum((weight_grad(tokens, dq), weight_grad(tokens, dk), weight_grad(tokens, dv), weight_grad(o, grad_y)), "sp")
        out_y = jnp.dot(o, w_o, preferred_element_type=F32).astype(BF16)
        grad_x = (back_proj(dq, w_q) + back_proj(dk, w_k) + back_proj(dv, w_v)).astype(BF16)
        return (out_y, grad_x) + tuple(grads)

    return jax.shard_map(local_layer, mesh=mesh, in_specs=(row_spec, P(), P(), P(), P(), row_spec),
                         out_specs=(row_spec, row_spec) + (grad_spec,) * 4, check_vma=False)
```

```python
import functools
import math
import jax
import jax.numpy as jnp
from jax import lax
from jax.experimental import pallas as pl
from jax.experimental.pallas import tpu as pltpu
from jax.sharding import PartitionSpec as P

HEAD_DIM = 128
BLOCK_LEN = 128
BF16 = jnp.bfloat16
F32 = jnp.float32
MESH = pl.DeviceIdType.MESH
CHUNKS = 8
TILE = 256
AT = (0, 1, 4, 8, 12, 15, 16)
VMEM_LIMIT = 64 * 1024 * 1024 - 1024 * 64


def dot(a, b):
    return lax.dot_general(a, b, (((1,), (0,)), ((), ())), preferred_element_type=F32)


def dot_nt(a, b):
    return lax.dot_general(a, b, (((1,), (1,)), ((), ())), preferred_element_type=F32)


def dot_tn(a, b):
    return lax.dot_general(a, b, (((0,), (0,)), ((), ())), preferred_element_type=F32)


def project_kernel(x_ref, dy_ref, wq_ref, wk_ref, wv_ref, wo_ref, q_ref, k_ref, v_ref, do_ref, tot_ref):
    @pl.when(pl.program_id(0) == 0)
    def _():
        tot_ref[...] = jnp.zeros_like(tot_ref)

    x = x_ref[...]
    q_ref[...] = dot(x, wq_ref[...]).astype(BF16)
    k_ref[...] = dot(x, wk_ref[...]).astype(BF16)
    v_ref[...] = dot(x, wv_ref[...]).astype(BF16)
    do_ref[...] = dot_nt(dy_ref[...], wo_ref[...]).astype(BF16)
    n_heads = x.shape[1] // HEAD_DIM
    for h in range(n_heads):
        cols = slice(h * HEAD_DIM, (h + 1) * HEAD_DIM)
        tot_ref[0, h] += dot_tn(k_ref[:, cols], v_ref[:, cols])
        tot_ref[1, h] += dot_tn(q_ref[:, cols], do_ref[:, cols])


def exchange_kernel(n_chips, tot_ref, init_ref, part, chip, recv, half, d2d_sem, send_sem, recv_sem, half_sem):
    me = lax.axis_index("sp")
    my_chip, core = me // 2, me % 2
    partner = my_chip * 2 + (1 - core)
    n_heads = tot_ref.shape[1]
    n_half = n_heads // 2
    barrier = pltpu.get_barrier_semaphore()
    peers = [partner] + [((my_chip + o) % n_chips) * 2 + core for o in range(1, n_chips)]
    for peer in peers:
        pl.semaphore_signal(barrier, inc=1, device_id={"sp": peer}, device_id_type=MESH)
    pl.semaphore_wait(barrier, len(peers))

    first = pltpu.make_async_remote_copy(tot_ref, part, d2d_sem.at[0], d2d_sem.at[1], device_id={"sp": partner}, device_id_type=MESH)
    first.start()
    first.wait()
    mine = pl.ds(core * n_half, n_half)
    chip[...] = tot_ref[:, mine] + part[:, mine]
    copies = []
    for o in range(1, n_chips):
        target = (my_chip + o) % n_chips
        kind = jnp.where(target > my_chip, 0, 1)
        copy = pltpu.make_async_remote_copy(chip.at[kind], recv.at[o - 1], send_sem.at[o - 1], recv_sem.at[o - 1],
                                            device_id={"sp": target * 2 + core}, device_id_type=MESH)
        copy.start()
        copies.append(copy)
    fwd = jnp.zeros_like(recv[0])
    rev = jnp.zeros_like(recv[0])
    for o in range(1, n_chips):
        copies[o - 1].wait()
        source = (my_chip + n_chips - o) % n_chips
        early = (source < my_chip).astype(F32)
        fwd = fwd + early * recv[o - 1]
        rev = rev + (1.0 - early) * recv[o - 1]
    half[0, 0] = fwd
    half[0, 1] = rev
    last = pltpu.make_async_remote_copy(half.at[0], half.at[1], half_sem.at[0], half_sem.at[1], device_id={"sp": partner}, device_id_type=MESH)
    last.start()
    last.wait()
    other = pl.ds((1 - core) * n_half, n_half)
    is_second = core.astype(F32)
    for slot, rows in ((0, mine), (1, other)):
        init_ref[0, rows] = half[slot, 0] + is_second * part[0, rows]
        init_ref[1, rows] = half[slot, 1] + (1.0 - is_second) * part[1, rows] + tot_ref[1, rows]


def layer_kernel(att_scale, n_chips, n_groups, q_ref, k_ref, v_ref, do_ref, x_ref, dy_ref, init_ref, wq_hbm, wk_hbm, wv_hbm, wo_hbm,
                 y_ref, dx_ref, grad_hbm, rows_hbm,
                 state, stage, part, pair, near, own, weights, tiles,
                 stage_sem, weight_sem, tile_sem, local_sem, send_sem, recv_sem):
    step = pl.program_id(0)
    me = lax.axis_index("sp")
    chip, core = me // 2, me % 2
    partner = chip * 2 + (1 - core)
    right_chip, left_chip, far_chip = (chip + 1) % n_chips, (chip + n_chips - 1) % n_chips, (chip + 2) % n_chips
    right, left = right_chip * 2 + core, left_chip * 2 + core
    n_chunks = CHUNKS
    att_steps = n_groups * n_chunks
    chunk, width = q_ref.shape
    core_rows = part.shape[1] // 2
    chip_rows = core_rows // n_chips
    half_rows = chip_rows // 2

    def rows_of(owner, half=None, of_core=None):
        base = (core if of_core is None else of_core) * core_rows + owner * chip_rows
        if half is None:
            return pl.ds(pl.multiple_of(base, half_rows), chip_rows)
        return pl.ds(pl.multiple_of(base + half * half_rows, half_rows), half_rows)

    def remote(kind, g, src, dst, target):
        return pltpu.make_async_remote_copy(src, dst, send_sem.at[kind, g], recv_sem.at[kind, g],
                                            device_id={"sp": target}, device_id_type=MESH)

    def message(kind, g):
        if kind == 0:
            other = pl.ds(pl.multiple_of((1 - core) * core_rows, core_rows), core_rows)
            return remote(0, g, part.at[g, other], pair.at[g % 2], partner)
        if kind in (1, 2):
            to, half = ((right, 0), (left, 1))[kind - 1]
            return remote(kind, g, part.at[g, rows_of(far_chip, half)], near.at[g, half], to)
        if kind in (3, 4):
            to, owner = ((right, right_chip), (left, left_chip))[kind - 3]
            return remote(kind, g, part.at[g, rows_of(owner)], own.at[g, kind - 3], to)
        if kind in (5, 6, 7):
            to = (right, left, partner)[kind - 5]
            return remote(kind, g, part.at[g, rows_of(chip)], grad_hbm.at[g, rows_of(chip)], to)
        if kind in (8, 9):
            to, rows = ((right, rows_of(left_chip, 0)), (left, rows_of(right_chip, 1)))[kind - 8]
        else:
            to, rows = partner, rows_of((left_chip, right_chip, far_chip)[kind - 10])
        return remote(kind, g, grad_hbm.at[g, rows], grad_hbm.at[g, rows], to)

    def local(g):
        return pltpu.make_async_copy(part.at[g, rows_of(chip)], grad_hbm.at[g, rows_of(chip)], local_sem.at[g])

    def event(offset):
        late = step - offset
        return (late >= 0) & (late < att_steps) & (late % n_chunks == 0), late // n_chunks

    @pl.when(step == 0)
    def _():
        barrier = pltpu.get_barrier_semaphore()
        for peer in (partner, right, left):
            pl.semaphore_signal(barrier, inc=1, device_id={"sp": peer}, device_id_type=MESH)
        pl.semaphore_wait(barrier, 3)
        for i, w in enumerate((wq_hbm, wk_hbm, wv_hbm, wo_hbm)):
            pltpu.make_async_copy(w, weights.at[i], weight_sem.at[i]).start()

    due, g0 = event(n_chunks + AT[0])

    @pl.when(due)
    def _():
        message(0, g0).start()

    due, g1 = event(n_chunks + AT[1])

    @pl.when(due)
    def _():
        message(0, g1).wait_recv()
        mine = pl.ds(pl.multiple_of(core * core_rows, core_rows), core_rows)
        part[g1, mine] += pair[g1 % 2]
        message(1, g1).start()
        message(2, g1).start()

    due, g2 = event(n_chunks + AT[2])

    @pl.when(due)
    def _():
        message(1, g2).wait_recv()
        message(2, g2).wait_recv()
        part[g2, rows_of(right_chip, 0)] += near[g2, 0]
        part[g2, rows_of(left_chip, 1)] += near[g2, 1]
        message(3, g2).start()
        message(4, g2).start()

    due, g3 = event(n_chunks + AT[3])

    @pl.when(due)
    def _():
        message(3, g3).wait_recv()
        message(4, g3).wait_recv()
        part[g3, rows_of(chip)] += own[g3, 0] + own[g3, 1]
        for kind in (5, 6, 7):
            message(kind, g3).start()
        local(g3).start()

    due, g4 = event(n_chunks + AT[4])

    @pl.when(due)
    def _():
        message(5, g4).wait_recv()
        message(6, g4).wait_recv()
        for kind in (8, 9, 10, 11):
            message(kind, g4).start()

    due, g5 = event(n_chunks + AT[5])

    @pl.when(due)
    def _():
        message(8, g5).wait_recv()
        message(9, g5).wait_recv()
        message(12, g5).start()

    due, g6 = event(n_chunks + AT[6])

    @pl.when(due)
    def _():
        for kind in (7, 10, 11, 12):
            message(kind, g6).wait_recv()
        local(g6).wait()
        for kind in range(13):
            message(kind, g6).wait_send()

    def put_stage(s):
        rows = pl.ds(pl.multiple_of((s % n_chunks) * chunk, chunk), chunk)
        return pltpu.make_async_copy(stage.at[s % 2], rows_hbm.at[s // n_chunks, rows], stage_sem.at[s % 2])

    tile_rows = tiles.shape[2]
    n_tiles = n_chunks * chunk // tile_rows

    def get_tile(t):
        rows = pl.ds(pl.multiple_of(t * tile_rows, tile_rows), tile_rows)
        return pltpu.make_async_copy(rows_hbm.at[:, rows], tiles.at[t % 2], tile_sem.at[t % 2])

    @pl.when((step >= 2) & (step < att_steps + 2))
    def _():
        put_stage(step - 2).wait()

    @pl.when(step < att_steps)
    def _():
        @pl.when(step % n_chunks == 0)
        def _():
            state[...] = init_ref[...]

        slot = step % 2
        row_id = lax.broadcasted_iota(jnp.int32, (BLOCK_LEN, BLOCK_LEN), 0)
        col_id = lax.broadcasted_iota(jnp.int32, (BLOCK_LEN, BLOCK_LEN), 1)
        causal = row_id >= col_id
        for h in range(width // HEAD_DIM):
            cols = slice(h * HEAD_DIM, (h + 1) * HEAD_DIM)
            s_run = state[0, h]
            r_run = state[1, h]
            for b in range(chunk // BLOCK_LEN):
                rows = slice(b * BLOCK_LEN, (b + 1) * BLOCK_LEN)
                q, k, v, do = q_ref[rows, cols], k_ref[rows, cols], v_ref[rows, cols], do_ref[rows, cols]
                r_run = r_run - dot_tn(q, do)
                s16, r16 = s_run.astype(BF16), r_run.astype(BF16)
                a = jnp.where(causal, dot_nt(q, k), 0.0).astype(BF16)
                e = jnp.where(causal, dot_nt(do, v), 0.0).astype(BF16)

                def put(i, value):
                    stage[slot, rows, i * width + h * HEAD_DIM:i * width + (h + 1) * HEAD_DIM] = (att_scale * value).astype(BF16)

                put(0, dot(e, k) + dot_nt(do, s16))
                put(1, dot_tn(e, q) + dot_nt(v, r16))
                put(2, dot_tn(a, do) + dot(k, r16))
                put(3, dot(a, v) + dot(q, s16))
                s_run = s_run + dot_tn(k, v)
            state[0, h] = s_run
            state[1, h] = r_run
        put_stage(step).start()
        g = step // n_chunks
        qkv = 3 * width

        @pl.when(step % n_chunks == 0)
        def _():
            part[g, :, :qkv] = dot_tn(x_ref[...], stage[slot, :, :qkv])
            part[g, :, qkv:] = dot_tn(dy_ref[...], stage[slot, :, qkv:])

        @pl.when(step % n_chunks > 0)
        def _():
            part[g, :, :qkv] += dot_tn(x_ref[...], stage[slot, :, :qkv])
            part[g, :, qkv:] += dot_tn(dy_ref[...], stage[slot, :, qkv:])

    tile = step - att_steps - 2

    @pl.when(tile == -1)
    def _():
        get_tile(0).start()
        for i, w in enumerate((wq_hbm, wk_hbm, wv_hbm, wo_hbm)):
            pltpu.make_async_copy(w, weights.at[i], weight_sem.at[i]).wait()

    @pl.when((tile >= 0) & (tile < n_tiles))
    def _():
        @pl.when(tile + 1 < n_tiles)
        def _():
            get_tile(tile + 1).start()

        get_tile(tile).wait()

        def gather(i):
            return jnp.concatenate([tiles[tile % 2, g, :, i * width:(i + 1) * width] for g in range(n_groups)], axis=1)

        dx_ref[...] = (dot_nt(gather(0), weights[0]) + dot_nt(gather(1), weights[1]) + dot_nt(gather(2), weights[2])).astype(BF16)
        y_ref[...] = dot(gather(3), weights[3]).astype(BF16)


def assemble_kernel(n_groups, grad_ref, wq_ref, wk_ref, wv_ref, wo_ref):
    width = grad_ref.shape[2] // 4
    for g in range(n_groups):
        cols = slice(g * width, (g + 1) * width)
        for i, out in enumerate((wq_ref, wk_ref, wv_ref)):
            out[:, cols] = grad_ref[g, :, i * width:(i + 1) * width]
        wo_ref[cols, :] = grad_ref[g, :, 3 * width:].T


def solution(mesh):
    n_seq = mesh.shape["sp"]
    row_spec = P(("dp", "sp"), None)
    grad_spec = P("dp", None)

    def local_layer(tokens, w_q, w_k, w_v, w_o, grad_y):
        n_rows, dim = tokens.shape
        n_heads = dim // HEAD_DIM
        att_scale = 1.0 / math.sqrt(n_rows * n_seq * HEAD_DIM)
        tile = 512
        rows_bf16 = jax.ShapeDtypeStruct((n_rows, dim), BF16)
        row_tile = pl.BlockSpec((tile, dim), lambda i: (i, 0))
        whole_w = pl.BlockSpec((dim, dim), lambda i: (0, 0), pipeline_mode=pl.Buffered(1))
        state_shape = (2, n_heads, HEAD_DIM, HEAD_DIM)
        q, k, v, do, totals = pl.pallas_call(
            project_kernel,
            grid=(n_rows // tile,),
            in_specs=[row_tile, row_tile] + [whole_w] * 4,
            out_specs=[row_tile] * 4 + [pl.BlockSpec(state_shape, lambda i: (0, 0, 0, 0))],
            out_shape=[rows_bf16] * 4 + [jax.ShapeDtypeStruct(state_shape, F32)],
            compiler_params=pltpu.CompilerParams(vmem_limit_bytes=VMEM_LIMIT, dimension_semantics=("arbitrary",)),
            name="project",
        )(tokens, grad_y, w_q, w_k, w_v, w_o)

        n_chips = n_seq // 2
        half_shape = (n_heads // 2, HEAD_DIM, HEAD_DIM)
        vmem = pl.BlockSpec(memory_space=pltpu.VMEM)
        init = pl.pallas_call(
            functools.partial(exchange_kernel, n_chips),
            in_specs=[vmem],
            out_specs=vmem,
            out_shape=jax.ShapeDtypeStruct(state_shape, F32),
            scratch_shapes=[
                pltpu.VMEM(state_shape, F32),
                pltpu.VMEM((2,) + half_shape, F32),
                pltpu.VMEM((n_chips - 1,) + half_shape, F32),
                pltpu.VMEM((2, 2) + half_shape, F32),
                pltpu.SemaphoreType.DMA((2,)),
                pltpu.SemaphoreType.DMA((n_chips - 1,)),
                pltpu.SemaphoreType.DMA((n_chips - 1,)),
                pltpu.SemaphoreType.DMA((2,)),
            ],
            compiler_params=pltpu.CompilerParams(vmem_limit_bytes=32 * 1024 * 1024, collective_id=0, has_side_effects=True),
            name="exchange",
        )(totals)

        width, chunk, tile_rows = 2 * HEAD_DIM, n_rows // CHUNKS, TILE
        n_groups, n_tiles = dim // width, n_rows // TILE
        att_steps = n_groups * CHUNKS
        n_steps = max(att_steps + 2 + n_tiles, att_steps + AT[6] + 1)

        def att(s):
            return jnp.minimum(s, att_steps - 1)

        def tile_index(s):
            return (jnp.clip(s - att_steps - 2, 0, n_tiles - 1), 0)

        col_tile = pl.BlockSpec((chunk, width), lambda s: (att(s) % CHUNKS, att(s) // CHUNKS))
        row_chunk = pl.BlockSpec((chunk, dim), lambda s: (att(s) % CHUNKS, 0))
        init_tile = pl.BlockSpec((2, width // HEAD_DIM, HEAD_DIM, HEAD_DIM), lambda s: (0, att(s) // CHUNKS, 0, 0))
        hbm = pl.BlockSpec(memory_space=pl.ANY)
        out_tile = pl.BlockSpec((tile_rows, dim), tile_index)
        chip_rows = dim // 2 // n_chips
        n_kinds = 13
        out_y, grad_x, grads, _ = pl.pallas_call(
            functools.partial(layer_kernel, att_scale, n_chips, n_groups),
            grid=(n_steps,),
            in_specs=[col_tile] * 4 + [row_chunk] * 2 + [init_tile] + [hbm] * 4,
            out_specs=[out_tile] * 2 + [hbm] * 2,
            out_shape=[rows_bf16] * 2 + [jax.ShapeDtypeStruct((n_groups, dim, 4 * width), F32),
                                         jax.ShapeDtypeStruct((n_groups, n_rows, 4 * width), BF16)],
            scratch_shapes=[
                pltpu.VMEM((2, width // HEAD_DIM, HEAD_DIM, HEAD_DIM), F32),
                pltpu.VMEM((2, chunk, 4 * width), BF16),
                pltpu.VMEM((n_groups, dim, 4 * width), F32),
                pltpu.VMEM((2, dim // 2, 4 * width), F32),
                pltpu.VMEM((n_groups, 2, chip_rows // 2, 4 * width), F32),
                pltpu.VMEM((n_groups, 2, chip_rows, 4 * width), F32),
                pltpu.VMEM((4, dim, dim), BF16),
                pltpu.VMEM((2, n_groups, tile_rows, 4 * width), BF16),
                pltpu.SemaphoreType.DMA((2,)),
                pltpu.SemaphoreType.DMA((4,)),
                pltpu.SemaphoreType.DMA((2,)),
                pltpu.SemaphoreType.DMA((n_groups,)),
                pltpu.SemaphoreType.DMA((n_kinds, n_groups)),
                pltpu.SemaphoreType.DMA((n_kinds, n_groups)),
            ],
            compiler_params=pltpu.CompilerParams(vmem_limit_bytes=VMEM_LIMIT, dimension_semantics=("arbitrary",), collective_id=1, has_side_effects=True),
            name="layer",
        )(q, k, v, do, tokens, grad_y, init, w_q, w_k, w_v, w_o)

        slab = 128
        grads = pl.pallas_call(
            functools.partial(assemble_kernel, n_groups),
            grid=(dim // slab,),
            in_specs=[pl.BlockSpec((n_groups, slab, 4 * width), lambda i: (0, i, 0))],
            out_specs=[pl.BlockSpec((slab, dim), lambda i: (i, 0))] * 3 + [pl.BlockSpec((dim, slab), lambda i: (0, i))],
            out_shape=[jax.ShapeDtypeStruct((dim, dim), F32)] * 4,
            compiler_params=pltpu.CompilerParams(vmem_limit_bytes=32 * 1024 * 1024, dimension_semantics=("arbitrary",)),
            name="assemble",
        )(grads)
        return (out_y, grad_x) + tuple(grads)

    return jax.shard_map(local_layer, mesh=mesh, in_specs=(row_spec, P(), P(), P(), P(), row_spec),
                         out_specs=(row_spec, row_spec) + (grad_spec,) * 4, check_vma=False)
```

```python
import functools
import math
import jax
import jax.numpy as jnp
from jax import lax
from jax.experimental import pallas as pl
from jax.experimental.pallas import tpu as pltpu
from jax.sharding import PartitionSpec as P

HEAD_DIM = 128
BLOCK_LEN = 128
BF16 = jnp.bfloat16
F32 = jnp.float32
MESH = pl.DeviceIdType.MESH
CHUNKS = 8
TILE = 256
FIRST = 5
AT0 = (0, 2, 5, 10, 15, 19, 21)
AT = (0, 1, 5, 11, 17, 22, 24)
XAT = (0, 1, 4, 5)
VMEM_LIMIT = 64 * 1024 * 1024 - 1024 * 64


def dot(a, b):
    return lax.dot_general(a, b, (((1,), (0,)), ((), ())), preferred_element_type=F32)


def dot_nt(a, b):
    return lax.dot_general(a, b, (((1,), (1,)), ((), ())), preferred_element_type=F32)


def dot_tn(a, b):
    return lax.dot_general(a, b, (((0,), (0,)), ((), ())), preferred_element_type=F32)


def project_rows(width, x, dy, w_q, w_k, w_v, w_o, z_ref, tot_ref):
    n_groups = z_ref.shape[0]
    for i, value in enumerate((dot(x, w_q), dot(x, w_k), dot(x, w_v), dot_nt(dy, w_o))):
        for g in range(n_groups):
            z_ref[g, :, i * width:(i + 1) * width] = value[:, g * width:(g + 1) * width].astype(BF16)
    per_group = width // HEAD_DIM
    for g in range(n_groups):
        for h in range(per_group):
            q, k, v, do = (z_ref[g, :, i * width + h * HEAD_DIM:i * width + (h + 1) * HEAD_DIM] for i in range(4))
            tot_ref[0, g * per_group + h] += dot_tn(k, v)
            tot_ref[1, g * per_group + h] += dot_tn(q, do)


def project_kernel(width, x_ref, dy_ref, wq_ref, wk_ref, wv_ref, wo_ref, z_ref, tot_ref):
    @pl.when(pl.program_id(0) == 0)
    def _():
        tot_ref[...] = jnp.zeros_like(tot_ref)

    project_rows(width, x_ref[...], dy_ref[...], wq_ref[...], wk_ref[...], wv_ref[...], wo_ref[...], z_ref, tot_ref)


def layer_kernel(att_scale, n_chips, n_groups, width, x_ref, dy_ref, tot_ref, early_hbm, wq_hbm, wk_hbm, wv_hbm, wo_hbm,
                 y_ref, dx_ref, grad_hbm, rows_hbm, late_hbm,
                 state, stage, part, pair, near, own, weights, zin, zout, mats, totals, x_part, x_chip, x_recv, x_half, x_init,
                 stage_sem, weight_sem, tile_sem, local_sem, send_sem, recv_sem, zin_sem, zout_sem, x_send, x_recv_sem):
    step = pl.program_id(0)
    me = lax.axis_index("sp")
    chip, core = me // 2, me % 2
    partner = chip * 2 + (1 - core)
    right_chip, left_chip, far_chip = (chip + 1) % n_chips, (chip + n_chips - 1) % n_chips, (chip + 2) % n_chips
    right, left = right_chip * 2 + core, left_chip * 2 + core
    n_chunks = CHUNKS
    att_steps = n_groups * n_chunks
    chunk = x_ref.shape[0]
    base = 2 * n_chunks
    n_early = early_hbm.shape[0]
    per_group = width // HEAD_DIM
    core_rows = part.shape[1] // 2
    chip_rows = core_rows // n_chips
    half_rows = chip_rows // 2

    def rows_of(owner, half=None, of_core=None):
        base = (core if of_core is None else of_core) * core_rows + owner * chip_rows
        if half is None:
            return pl.ds(pl.multiple_of(base, half_rows), chip_rows)
        return pl.ds(pl.multiple_of(base + half * half_rows, half_rows), half_rows)

    def remote(kind, g, src, dst, target):
        return pltpu.make_async_remote_copy(src, dst, send_sem.at[kind, g], recv_sem.at[kind, g],
                                            device_id={"sp": target}, device_id_type=MESH)

    def message(kind, g):
        if kind == 0:
            other = pl.ds(pl.multiple_of((1 - core) * core_rows, core_rows), core_rows)
            return remote(0, g, part.at[g, other], pair.at[g % 2], partner)
        if kind in (1, 2):
            to, half = ((right, 0), (left, 1))[kind - 1]
            return remote(kind, g, part.at[g, rows_of(far_chip, half)], near.at[g % 2, half], to)
        if kind in (3, 4):
            to, owner = ((right, right_chip), (left, left_chip))[kind - 3]
            return remote(kind, g, part.at[g, rows_of(owner)], own.at[g % 2, kind - 3], to)
        if kind in (5, 6, 7):
            to = (right, left, partner)[kind - 5]
            return remote(kind, g, part.at[g, rows_of(chip)], grad_hbm.at[g, rows_of(chip)], to)
        if kind in (8, 9):
            to, rows = ((right, rows_of(left_chip, 0)), (left, rows_of(right_chip, 1)))[kind - 8]
        else:
            to, rows = partner, rows_of((left_chip, right_chip, far_chip)[kind - 10])
        return remote(kind, g, grad_hbm.at[g, rows], grad_hbm.at[g, rows], to)

    def local(g):
        return pltpu.make_async_copy(part.at[g, rows_of(chip)], grad_hbm.at[g, rows_of(chip)], local_sem.at[g])

    def event(i):
        zeroth = step == FIRST + n_chunks + AT0[i]
        late = step - base - AT[i]
        due = (late >= n_chunks) & (late < att_steps) & (late % n_chunks == 0)
        return zeroth | due, jnp.where(zeroth, 0, late // n_chunks)

    @pl.when(step == 0)
    def _():
        barrier = pltpu.get_barrier_semaphore()
        peers = [partner] + [((chip + o) % n_chips) * 2 + core for o in range(1, n_chips)]
        for peer in peers:
            pl.semaphore_signal(barrier, inc=1, device_id={"sp": peer}, device_id_type=MESH)
        for i, w in enumerate((wq_hbm, wk_hbm, wv_hbm, wo_hbm)):
            pltpu.make_async_copy(w, weights.at[i], weight_sem.at[i]).start()
        totals[0] = tot_ref[...]
        totals[1] = jnp.zeros_like(totals[1])
        pl.semaphore_wait(barrier, len(peers))
        for i, w in enumerate((wq_hbm, wk_hbm, wv_hbm, wo_hbm)):
            pltpu.make_async_copy(w, weights.at[i], weight_sem.at[i]).wait()

    n_half = x_chip.shape[2]
    mine = pl.ds(core * n_half, n_half)
    other = pl.ds((1 - core) * n_half, n_half)

    def x_message(kind, f):
        if kind == 0:
            src, dst, to = totals.at[f], x_part.at[f], partner
        elif kind < n_chips:
            target = (chip + kind) % n_chips
            src, dst, to = x_chip.at[f, jnp.where(target > chip, 0, 1)], x_recv.at[f, kind - 1], target * 2 + core
        else:
            src, dst, to = x_half.at[f, 0], x_half.at[f, 1], partner
        return pltpu.make_async_remote_copy(src, dst, x_send.at[kind, f], x_recv_sem.at[kind, f], device_id={"sp": to}, device_id_type=MESH)

    def x_event(offset):
        late = step - offset
        return (late >= 0) & (late < 4 * n_chunks) & (late % (2 * n_chunks) == 0), late // (2 * n_chunks)

    due, f0 = x_event(XAT[0])

    @pl.when(due)
    def _():
        x_message(0, f0).start()

    due, f1 = x_event(XAT[1])

    @pl.when(due)
    def _():
        x_message(0, f1).wait_recv()
        x_chip[f1] = totals[f1, :, mine] + x_part[f1, :, mine]
        for o in range(1, n_chips):
            x_message(o, f1).start()

    due, f2 = x_event(XAT[2])

    @pl.when(due)
    def _():
        fwd = jnp.zeros(x_recv.shape[2:], F32)
        rev = jnp.zeros(x_recv.shape[2:], F32)
        for o in range(1, n_chips):
            x_message(o, f2).wait_recv()
            early = ((chip + n_chips - o) % n_chips < chip).astype(F32)
            fwd = fwd + early * x_recv[f2, o - 1]
            rev = rev + (1.0 - early) * x_recv[f2, o - 1]
        x_half[f2, 0, 0] = fwd
        x_half[f2, 0, 1] = rev
        x_message(n_chips, f2).start()

    due, f3 = x_event(XAT[3])

    @pl.when(due)
    def _():
        x_message(n_chips, f3).wait_recv()
        is_second = core.astype(F32)
        for slot, heads in ((0, mine), (1, other)):
            x_init[f3, 0, heads] = x_half[f3, slot, 0] + is_second * x_part[f3, 0, heads]
            x_init[f3, 1, heads] = x_half[f3, slot, 1] + (1.0 - is_second) * x_part[f3, 1, heads] + totals[f3, 1, heads]
        for kind in range(n_chips + 1):
            x_message(kind, f3).wait_send()

    due, g0 = event(0)

    @pl.when(due)
    def _():
        message(0, g0).start()

    due, g1 = event(1)

    @pl.when(due)
    def _():
        message(0, g1).wait_recv()
        mine = pl.ds(pl.multiple_of(core * core_rows, core_rows), core_rows)
        part[g1, mine] += pair[g1 % 2]
        message(1, g1).start()
        message(2, g1).start()

    due, g2 = event(2)

    @pl.when(due)
    def _():
        message(1, g2).wait_recv()
        message(2, g2).wait_recv()
        part[g2, rows_of(right_chip, 0)] += near[g2 % 2, 0]
        part[g2, rows_of(left_chip, 1)] += near[g2 % 2, 1]
        message(3, g2).start()
        message(4, g2).start()

    due, g3 = event(3)

    @pl.when(due)
    def _():
        message(3, g3).wait_recv()
        message(4, g3).wait_recv()
        part[g3, rows_of(chip)] += own[g3 % 2, 0] + own[g3 % 2, 1]
        for kind in (5, 6, 7):
            message(kind, g3).start()
        local(g3).start()

    due, g4 = event(4)

    @pl.when(due)
    def _():
        message(5, g4).wait_recv()
        message(6, g4).wait_recv()
        for kind in (8, 9, 10, 11):
            message(kind, g4).start()

    due, g5 = event(5)

    @pl.when(due)
    def _():
        message(8, g5).wait_recv()
        message(9, g5).wait_recv()
        message(12, g5).start()

    due, g6 = event(6)

    @pl.when(due)
    def _():
        for kind in (7, 10, 11, 12):
            message(kind, g6).wait_recv()
        local(g6).wait()
        for kind in range(13):
            message(kind, g6).wait_send()

    def put_stage(s):
        rows = pl.ds(pl.multiple_of((s % n_chunks) * chunk, chunk), chunk)
        return pltpu.make_async_copy(stage.at[s % 2], rows_hbm.at[s // n_chunks, rows], stage_sem.at[s % 2])

    tile_rows = y_ref.shape[0]
    n_tiles = n_chunks * chunk // tile_rows
    per_slab = chunk // tile_rows

    def tile_of(g):
        return g // per_slab, pl.ds(g % per_slab * tile_rows, tile_rows)

    def get_tile(i, act):
        rows = pl.ds(pl.multiple_of(i * tile_rows, tile_rows), tile_rows)
        for g in range(n_groups):
            slab, part_of_slab = tile_of(g)
            act(pltpu.make_async_copy(rows_hbm.at[g, rows], zout.at[i % 2, slab, part_of_slab], tile_sem.at[i % 2, g]))

    def put_z(p):
        rows = pl.ds(pl.multiple_of(p * chunk, chunk), chunk)
        return pltpu.make_async_copy(zout.at[p % 2], late_hbm.at[:, rows], zout_sem.at[p % 2])

    def get_z(t, act):
        g = t // n_chunks
        rows = pl.ds(pl.multiple_of((t % n_chunks) * chunk, chunk), chunk)

        @pl.when(g < n_early)
        def _():
            act(pltpu.make_async_copy(early_hbm.at[jnp.minimum(g, n_early - 1), rows], zin.at[t % 2], zin_sem.at[t % 2]))

        @pl.when(g >= n_early)
        def _():
            act(pltpu.make_async_copy(late_hbm.at[jnp.maximum(g - n_early, 0), rows], zin.at[t % 2], zin_sem.at[t % 2]))

    before = step < FIRST
    p = jnp.where(before, step, step - n_chunks)
    is_project = before | ((step >= FIRST + n_chunks) & (step < base))

    @pl.when((is_project & (p >= 2)) | (step == base) | (step == base + 1))
    def _():
        put_z(p - 2).wait()

    @pl.when(is_project)
    def _():
        late_cols = slice(n_early * width, n_groups * width)
        project_rows(width, x_ref[...], dy_ref[...], weights[0, :, late_cols], weights[1, :, late_cols], weights[2, :, late_cols],
                     weights[3, late_cols, :], zout.at[p % 2], totals.at[1])
        put_z(p).start()

    t = jnp.where(step < base, step - FIRST, step - n_chunks)
    is_attention = ((step >= FIRST) & (step < FIRST + n_chunks)) | ((step >= base) & (step < n_chunks + att_steps))

    @pl.when((step == FIRST - 1) | (is_attention & (t < att_steps - 1)))
    def _():
        get_z(t + 1, lambda copy: copy.start())

    @pl.when((is_attention & (t >= 2)) | (step == n_chunks + att_steps) | (step == n_chunks + att_steps + 1))
    def _():
        put_stage(t - 2).wait()

    @pl.when(is_attention)
    def _():
        g = t // n_chunks

        @pl.when(t % n_chunks == 0)
        def _():
            state[...] = x_init[g // n_early, :, pl.ds((g % n_early) * per_group, per_group)]

        get_z(t, lambda copy: copy.wait())
        slot = t % 2
        row_id = lax.broadcasted_iota(jnp.int32, (BLOCK_LEN, BLOCK_LEN), 0)
        col_id = lax.broadcasted_iota(jnp.int32, (BLOCK_LEN, BLOCK_LEN), 1)
        causal = row_id >= col_id
        n_blocks = chunk // BLOCK_LEN
        pairs = [(h, b) for h in range(per_group) for b in range(n_blocks)]

        def block(i, h, b):
            start = i * width + h * HEAD_DIM
            return zin[slot, b * BLOCK_LEN:(b + 1) * BLOCK_LEN, start:start + HEAD_DIM]

        def beside(left, right):
            return jnp.concatenate([left, right], axis=1)

        def above(top, bottom):
            return jnp.concatenate([top, bottom], axis=0)

        for n, (h, b) in enumerate(pairs):
            q, k, v, do = (block(i, h, b) for i in range(4))
            k_t = k.T
            s16 = state[0, h].astype(BF16)
            state[0, h] += dot(k_t, v)
            r_run = state[1, h] - dot_tn(q, do)
            state[1, h] = r_run
            r16 = r_run.astype(BF16)
            mats[n, 0], mats[n, 1], mats[n, 2], mats[n, 3] = s16, s16.T, r16, r16.T
            a = jnp.where(causal, dot(q, k_t), 0.0).astype(BF16)
            e = jnp.where(causal, dot_nt(do, v), 0.0).astype(BF16)
            mats[n, 4], mats[n, 5], mats[n, 6], mats[n, 7] = a, a.T, e, e.T
        for n, (h, b) in enumerate(pairs):
            q, k, v, do = (block(i, h, b) for i in range(4))
            s16, s16_t, r16, r16_t, a, a_t, e, e_t = (mats[n, i] for i in range(8))
            values = (dot(beside(e, do), above(k, s16_t)), dot(beside(e_t, v), above(q, r16_t)),
                      dot(beside(a_t, k), above(do, r16)), dot(beside(a, q), above(v, s16)))
            for i, value in enumerate(values):
                start = i * width + h * HEAD_DIM
                stage[slot, b * BLOCK_LEN:(b + 1) * BLOCK_LEN, start:start + HEAD_DIM] = (att_scale * value).astype(BF16)
        put_stage(t).start()
        qkv = 3 * width

        @pl.when(t % n_chunks == 0)
        def _():
            part[g, :, :qkv] = dot_tn(x_ref[...], stage[slot, :, :qkv])
            part[g, :, qkv:] = dot_tn(dy_ref[...], stage[slot, :, qkv:])

        @pl.when(t % n_chunks > 0)
        def _():
            part[g, :, :qkv] += dot_tn(x_ref[...], stage[slot, :, :qkv])
            part[g, :, qkv:] += dot_tn(dy_ref[...], stage[slot, :, qkv:])

    tile = step - n_chunks - att_steps - 2

    @pl.when(tile == -1)
    def _():
        get_tile(0, lambda copy: copy.start())

    @pl.when((tile >= 0) & (tile < n_tiles))
    def _():
        @pl.when(tile + 1 < n_tiles)
        def _():
            get_tile(tile + 1, lambda copy: copy.start())

        get_tile(tile, lambda copy: copy.wait())

        def gather(i):
            return jnp.concatenate([zout[(tile % 2,) + tile_of(g) + (slice(i * width, (i + 1) * width),)] for g in range(n_groups)], axis=1)

        dx_ref[...] = (dot_nt(gather(0), weights[0]) + dot_nt(gather(1), weights[1]) + dot_nt(gather(2), weights[2])).astype(BF16)
        y_ref[...] = dot(gather(3), weights[3]).astype(BF16)


def assemble_kernel(n_groups, grad_ref, wq_ref, wk_ref, wv_ref, wo_ref):
    width = grad_ref.shape[2] // 4
    for g in range(n_groups):
        cols = slice(g * width, (g + 1) * width)
        for i, out in enumerate((wq_ref, wk_ref, wv_ref)):
            out[:, cols] = grad_ref[g, :, i * width:(i + 1) * width]
        wo_ref[cols, :] = grad_ref[g, :, 3 * width:].T


def solution(mesh):
    n_seq = mesh.shape["sp"]
    row_spec = P(("dp", "sp"), None)
    grad_spec = P("dp", None)

    def local_layer(tokens, w_q, w_k, w_v, w_o, grad_y):
        n_rows, dim = tokens.shape
        n_heads = dim // HEAD_DIM
        att_scale = 1.0 / math.sqrt(n_rows * n_seq * HEAD_DIM)
        tile = 512
        n_chips = n_seq // 2
        width, chunk, tile_rows = 2 * HEAD_DIM, n_rows // CHUNKS, TILE
        n_groups, n_tiles = dim // width, n_rows // TILE
        n_early = n_groups // 2
        early_cols = n_early * width
        rows_bf16 = jax.ShapeDtypeStruct((n_rows, dim), BF16)
        row_tile = pl.BlockSpec((tile, dim), lambda i: (i, 0))
        some_cols = pl.BlockSpec((dim, early_cols), lambda i: (0, 0), pipeline_mode=pl.Buffered(1))
        some_rows = pl.BlockSpec((early_cols, dim), lambda i: (0, 0), pipeline_mode=pl.Buffered(1))
        state_shape = (2, n_heads // 2, HEAD_DIM, HEAD_DIM)
        whole_state = pl.BlockSpec(state_shape, lambda i: (0, 0, 0, 0))
        half_rows = jax.ShapeDtypeStruct((n_early, n_rows, 4 * width), BF16)
        early, totals = pl.pallas_call(
            functools.partial(project_kernel, width),
            grid=(n_rows // tile,),
            in_specs=[row_tile, row_tile] + [some_cols] * 3 + [some_rows],
            out_specs=[pl.BlockSpec((n_early, tile, 4 * width), lambda i: (0, i, 0)), whole_state],
            out_shape=[half_rows, jax.ShapeDtypeStruct(state_shape, F32)],
            compiler_params=pltpu.CompilerParams(vmem_limit_bytes=VMEM_LIMIT, dimension_semantics=("arbitrary",)),
            name="project",
        )(tokens, grad_y, w_q, w_k, w_v, w_o)

        att_steps = n_groups * CHUNKS
        n_steps = CHUNKS + max(att_steps + 2 + n_tiles, att_steps + AT[6] + 1)

        def tile_index(s):
            return (jnp.clip(s - CHUNKS - att_steps - 2, 0, n_tiles - 1), 0)

        def chunk_index(s):
            late = jnp.minimum(s, CHUNKS + att_steps - 1) % CHUNKS
            return (jnp.where((s >= FIRST) & (s < FIRST + CHUNKS), s - FIRST, late), 0)

        row_chunk = pl.BlockSpec((chunk, dim), chunk_index)
        hbm = pl.BlockSpec(memory_space=pl.ANY)
        out_tile = pl.BlockSpec((tile_rows, dim), tile_index)
        chip_rows = dim // 2 // n_chips
        n_kinds = 13
        head_shape = (n_heads // 4, HEAD_DIM, HEAD_DIM)
        out_y, grad_x, grads, _, _ = pl.pallas_call(
            functools.partial(layer_kernel, att_scale, n_chips, n_groups, width),
            grid=(n_steps,),
            in_specs=[row_chunk] * 2 + [whole_state] + [hbm] * 5,
            out_specs=[out_tile] * 2 + [hbm] * 3,
            out_shape=[rows_bf16] * 2 + [jax.ShapeDtypeStruct((n_groups, dim, 4 * width), F32),
                                         jax.ShapeDtypeStruct((n_groups, n_rows, 4 * width), BF16), half_rows],
            scratch_shapes=[
                pltpu.VMEM((2, width // HEAD_DIM, HEAD_DIM, HEAD_DIM), F32),
                pltpu.VMEM((2, chunk, 4 * width), BF16),
                pltpu.VMEM((n_groups, dim, 4 * width), F32),
                pltpu.VMEM((2, dim // 2, 4 * width), F32),
                pltpu.VMEM((2, 2, chip_rows // 2, 4 * width), F32),
                pltpu.VMEM((2, 2, chip_rows, 4 * width), F32),
                pltpu.VMEM((4, dim, dim), BF16),
                pltpu.VMEM((2, chunk, 4 * width), BF16),
                pltpu.VMEM((2, n_early, chunk, 4 * width), BF16),
                pltpu.VMEM((width // HEAD_DIM * (chunk // BLOCK_LEN), 8, BLOCK_LEN, HEAD_DIM), BF16),
                pltpu.VMEM((2,) + state_shape, F32),
                pltpu.VMEM((2,) + state_shape, F32),
                pltpu.VMEM((2, 2) + head_shape, F32),
                pltpu.VMEM((2, n_chips - 1) + head_shape, F32),
                pltpu.VMEM((2, 2, 2) + head_shape, F32),
                pltpu.VMEM((2,) + state_shape, F32),
                pltpu.SemaphoreType.DMA((2,)),
                pltpu.SemaphoreType.DMA((4,)),
                pltpu.SemaphoreType.DMA((2, n_groups)),
                pltpu.SemaphoreType.DMA((n_groups,)),
                pltpu.SemaphoreType.DMA((n_kinds, n_groups)),
                pltpu.SemaphoreType.DMA((n_kinds, n_groups)),
                pltpu.SemaphoreType.DMA((2,)),
                pltpu.SemaphoreType.DMA((2,)),
                pltpu.SemaphoreType.DMA((n_chips + 1, 2)),
                pltpu.SemaphoreType.DMA((n_chips + 1, 2)),
            ],
            compiler_params=pltpu.CompilerParams(vmem_limit_bytes=VMEM_LIMIT, dimension_semantics=("arbitrary",), collective_id=1, has_side_effects=True),
            name="layer",
        )(tokens, grad_y, totals, early, w_q, w_k, w_v, w_o)

        slab = 128
        grads = pl.pallas_call(
            functools.partial(assemble_kernel, n_groups),
            grid=(dim // slab,),
            in_specs=[pl.BlockSpec((n_groups, slab, 4 * width), lambda i: (0, i, 0))],
            out_specs=[pl.BlockSpec((slab, dim), lambda i: (i, 0))] * 3 + [pl.BlockSpec((dim, slab), lambda i: (0, i))],
            out_shape=[jax.ShapeDtypeStruct((dim, dim), F32)] * 4,
            compiler_params=pltpu.CompilerParams(vmem_limit_bytes=32 * 1024 * 1024, dimension_semantics=("arbitrary",)),
            name="assemble",
        )(grads)
        return (out_y, grad_x) + tuple(grads)

    return jax.shard_map(local_layer, mesh=mesh, in_specs=(row_spec, P(), P(), P(), P(), row_spec),
                         out_specs=(row_spec, row_spec) + (grad_spec,) * 4, check_vma=False)
```

```python
import functools
import math
import jax
import jax.numpy as jnp
from jax import lax
from jax.experimental import pallas as pl
from jax.experimental.pallas import tpu as pltpu
from jax.sharding import PartitionSpec as P

HEAD_DIM = 128
BLOCK_LEN = 128
BF16 = jnp.bfloat16
F32 = jnp.float32
MESH = pl.DeviceIdType.MESH
CHUNKS = 8
TILE = 256
FIRST = 5
AT0 = (0, 2, 5, 10, 15, 19, 21)
AT = (0, 1, 5, 11, 17, 22, 24)
XAT = (0, 1, 4, 5)
VMEM_LIMIT = 64 * 1024 * 1024 - 1024 * 64


def dot(a, b):
    return lax.dot_general(a, b, (((1,), (0,)), ((), ())), preferred_element_type=F32)


def dot_nt(a, b):
    return lax.dot_general(a, b, (((1,), (1,)), ((), ())), preferred_element_type=F32)


def dot_tn(a, b):
    return lax.dot_general(a, b, (((0,), (0,)), ((), ())), preferred_element_type=F32)


def project_rows(width, x, dy, w_q, w_k, w_v, w_o, z_ref, tot_ref):
    n_groups = z_ref.shape[0]
    for i, value in enumerate((dot(x, w_q), dot(x, w_k), dot(x, w_v), dot_nt(dy, w_o))):
        for g in range(n_groups):
            z_ref[g, :, i * width:(i + 1) * width] = value[:, g * width:(g + 1) * width].astype(BF16)
    per_group = width // HEAD_DIM
    for g in range(n_groups):
        for h in range(per_group):
            q, k, v, do = (z_ref[g, :, i * width + h * HEAD_DIM:i * width + (h + 1) * HEAD_DIM] for i in range(4))
            tot_ref[0, g * per_group + h] += dot_tn(k, v)
            tot_ref[1, g * per_group + h] += dot_tn(q, do)


def project_kernel(width, x_ref, dy_ref, wq_ref, wk_ref, wv_ref, wo_ref, z_ref, tot_ref):
    @pl.when(pl.program_id(0) == 0)
    def _():
        tot_ref[...] = jnp.zeros_like(tot_ref)

    project_rows(width, x_ref[...], dy_ref[...], wq_ref[...], wk_ref[...], wv_ref[...], wo_ref[...], z_ref, tot_ref)


def layer_kernel(att_scale, n_chips, n_groups, width, x_ref, dy_ref, tot_ref, early_hbm, wq_hbm, wk_hbm, wv_hbm, wo_hbm,
                 y_ref, dx_ref, grad_hbm, rows_hbm, late_hbm,
                 state, stage, part, pair, near, own, weights, zin, zout, mats, totals, x_part, x_chip, x_recv, x_half, x_init,
                 stage_sem, weight_sem, tile_sem, local_sem, send_sem, recv_sem, zin_sem, zout_sem, x_send, x_recv_sem):
    step = pl.program_id(0)
    me = lax.axis_index("sp")
    chip, core = me // 2, me % 2
    partner = chip * 2 + (1 - core)
    right_chip, left_chip, far_chip = (chip + 1) % n_chips, (chip + n_chips - 1) % n_chips, (chip + 2) % n_chips
    right, left = right_chip * 2 + core, left_chip * 2 + core
    n_chunks = CHUNKS
    att_steps = n_groups * n_chunks
    chunk = x_ref.shape[0]
    base = 2 * n_chunks
    n_early = early_hbm.shape[0]
    per_group = width // HEAD_DIM
    core_rows = part.shape[1] // 2
    chip_rows = core_rows // n_chips
    half_rows = chip_rows // 2

    def rows_of(owner, half=None, of_core=None):
        base = (core if of_core is None else of_core) * core_rows + owner * chip_rows
        if half is None:
            return pl.ds(pl.multiple_of(base, half_rows), chip_rows)
        return pl.ds(pl.multiple_of(base + half * half_rows, half_rows), half_rows)

    def remote(kind, g, src, dst, target):
        return pltpu.make_async_remote_copy(src, dst, send_sem.at[kind, g], recv_sem.at[kind, g],
                                            device_id={"sp": target}, device_id_type=MESH)

    def message(kind, g):
        if kind == 0:
            other = pl.ds(pl.multiple_of((1 - core) * core_rows, core_rows), core_rows)
            return remote(0, g, part.at[g, other], pair.at[g % 2], partner)
        if kind in (1, 2):
            to, half = ((right, 0), (left, 1))[kind - 1]
            return remote(kind, g, part.at[g, rows_of(far_chip, half)], near.at[g % 2, half], to)
        if kind in (3, 4):
            to, owner = ((right, right_chip), (left, left_chip))[kind - 3]
            return remote(kind, g, part.at[g, rows_of(owner)], own.at[g % 2, kind - 3], to)
        if kind in (5, 6, 7):
            to = (right, left, partner)[kind - 5]
            return remote(kind, g, part.at[g, rows_of(chip)], grad_hbm.at[g, rows_of(chip)], to)
        if kind in (8, 9):
            to, rows = ((right, rows_of(left_chip, 0)), (left, rows_of(right_chip, 1)))[kind - 8]
        else:
            to, rows = partner, rows_of((left_chip, right_chip, far_chip)[kind - 10])
        return remote(kind, g, grad_hbm.at[g, rows], grad_hbm.at[g, rows], to)

    def local(g):
        return pltpu.make_async_copy(part.at[g, rows_of(chip)], grad_hbm.at[g, rows_of(chip)], local_sem.at[g])

    def event(i):
        zeroth = step == FIRST + n_chunks + AT0[i]
        late = step - base - AT[i]
        due = (late >= n_chunks) & (late < att_steps) & (late % n_chunks == 0)
        return zeroth | due, jnp.where(zeroth, 0, late // n_chunks)

    @pl.when(step == 0)
    def _():
        barrier = pltpu.get_barrier_semaphore()
        peers = [partner] + [((chip + o) % n_chips) * 2 + core for o in range(1, n_chips)]
        for peer in peers:
            pl.semaphore_signal(barrier, inc=1, device_id={"sp": peer}, device_id_type=MESH)
        for i, w in enumerate((wq_hbm, wk_hbm, wv_hbm, wo_hbm)):
            pltpu.make_async_copy(w, weights.at[i], weight_sem.at[i]).start()
        totals[0] = tot_ref[...]
        totals[1] = jnp.zeros_like(totals[1])
        pl.semaphore_wait(barrier, len(peers))
        for i, w in enumerate((wq_hbm, wk_hbm, wv_hbm, wo_hbm)):
            pltpu.make_async_copy(w, weights.at[i], weight_sem.at[i]).wait()

    n_half = x_chip.shape[2]
    mine = pl.ds(core * n_half, n_half)
    other = pl.ds((1 - core) * n_half, n_half)

    def x_message(kind, f):
        if kind == 0:
            src, dst, to = totals.at[f], x_part.at[f], partner
        elif kind < n_chips:
            target = (chip + kind) % n_chips
            src, dst, to = x_chip.at[f, jnp.where(target > chip, 0, 1)], x_recv.at[f, kind - 1], target * 2 + core
        else:
            src, dst, to = x_half.at[f, 0], x_half.at[f, 1], partner
        return pltpu.make_async_remote_copy(src, dst, x_send.at[kind, f], x_recv_sem.at[kind, f], device_id={"sp": to}, device_id_type=MESH)

    def x_event(offset):
        late = step - offset
        return (late >= 0) & (late < 4 * n_chunks) & (late % (2 * n_chunks) == 0), late // (2 * n_chunks)

    due, f0 = x_event(XAT[0])

    @pl.when(due)
    def _():
        x_message(0, f0).start()

    due, f1 = x_event(XAT[1])

    @pl.when(due)
    def _():
        x_message(0, f1).wait_recv()
        x_chip[f1] = totals[f1, :, mine] + x_part[f1, :, mine]
        for o in range(1, n_chips):
            x_message(o, f1).start()

    due, f2 = x_event(XAT[2])

    @pl.when(due)
    def _():
        fwd = jnp.zeros(x_recv.shape[2:], F32)
        rev = jnp.zeros(x_recv.shape[2:], F32)
        for o in range(1, n_chips):
            x_message(o, f2).wait_recv()
            early = ((chip + n_chips - o) % n_chips < chip).astype(F32)
            fwd = fwd + early * x_recv[f2, o - 1]
            rev = rev + (1.0 - early) * x_recv[f2, o - 1]
        x_half[f2, 0, 0] = fwd
        x_half[f2, 0, 1] = rev
        x_message(n_chips, f2).start()

    due, f3 = x_event(XAT[3])

    @pl.when(due)
    def _():
        x_message(n_chips, f3).wait_recv()
        is_second = core.astype(F32)
        for slot, heads in ((0, mine), (1, other)):
            x_init[f3, 0, heads] = x_half[f3, slot, 0] + is_second * x_part[f3, 0, heads]
            x_init[f3, 1, heads] = x_half[f3, slot, 1] + (1.0 - is_second) * x_part[f3, 1, heads] + totals[f3, 1, heads]
        for kind in range(n_chips + 1):
            x_message(kind, f3).wait_send()

    due, g0 = event(0)

    @pl.when(due)
    def _():
        message(0, g0).start()

    due, g1 = event(1)

    @pl.when(due)
    def _():
        message(0, g1).wait_recv()
        mine = pl.ds(pl.multiple_of(core * core_rows, core_rows), core_rows)
        part[g1, mine] += pair[g1 % 2]
        message(1, g1).start()
        message(2, g1).start()

    due, g2 = event(2)

    @pl.when(due)
    def _():
        message(1, g2).wait_recv()
        message(2, g2).wait_recv()
        part[g2, rows_of(right_chip, 0)] += near[g2 % 2, 0]
        part[g2, rows_of(left_chip, 1)] += near[g2 % 2, 1]
        message(3, g2).start()
        message(4, g2).start()

    due, g3 = event(3)

    @pl.when(due)
    def _():
        message(3, g3).wait_recv()
        message(4, g3).wait_recv()
        part[g3, rows_of(chip)] += own[g3 % 2, 0] + own[g3 % 2, 1]
        for kind in (5, 6, 7):
            message(kind, g3).start()
        local(g3).start()

    due, g4 = event(4)

    @pl.when(due)
    def _():
        message(5, g4).wait_recv()
        message(6, g4).wait_recv()
        for kind in (8, 9, 10, 11):
            message(kind, g4).start()

    due, g5 = event(5)

    @pl.when(due)
    def _():
        message(8, g5).wait_recv()
        message(9, g5).wait_recv()
        message(12, g5).start()

    due, g6 = event(6)

    @pl.when(due)
    def _():
        for kind in (7, 10, 11, 12):
            message(kind, g6).wait_recv()
        local(g6).wait()
        for kind in range(13):
            message(kind, g6).wait_send()

    def put_stage(s):
        rows = pl.ds(pl.multiple_of((s % n_chunks) * chunk, chunk), chunk)
        return pltpu.make_async_copy(stage.at[s % 2], rows_hbm.at[s // n_chunks, rows], stage_sem.at[s % 2])

    tile_rows = y_ref.shape[0]
    n_tiles = n_chunks * chunk // tile_rows
    per_slab = chunk // tile_rows

    def tile_of(g):
        return g // per_slab, pl.ds(g % per_slab * tile_rows, tile_rows)

    def get_tile(i, act):
        rows = pl.ds(pl.multiple_of(i * tile_rows, tile_rows), tile_rows)
        for g in range(n_groups):
            slab, part_of_slab = tile_of(g)
            act(pltpu.make_async_copy(rows_hbm.at[g, rows], zout.at[i % 2, slab, part_of_slab], tile_sem.at[i % 2, g]))

    def put_z(p):
        rows = pl.ds(pl.multiple_of(p * chunk, chunk), chunk)
        return pltpu.make_async_copy(zout.at[p % 2], late_hbm.at[:, rows], zout_sem.at[p % 2])

    def get_z(t, act):
        g = t // n_chunks
        rows = pl.ds(pl.multiple_of((t % n_chunks) * chunk, chunk), chunk)

        @pl.when(g < n_early)
        def _():
            act(pltpu.make_async_copy(early_hbm.at[jnp.minimum(g, n_early - 1), rows], zin.at[t % 2], zin_sem.at[t % 2]))

        @pl.when(g >= n_early)
        def _():
            act(pltpu.make_async_copy(late_hbm.at[jnp.maximum(g - n_early, 0), rows], zin.at[t % 2], zin_sem.at[t % 2]))

    before = step < FIRST
    p = jnp.where(before, step, step - n_chunks)
    is_project = before | ((step >= FIRST + n_chunks) & (step < base))

    @pl.when((is_project & (p >= 2)) | (step == base) | (step == base + 1))
    def _():
        put_z(p - 2).wait()

    @pl.when(is_project)
    def _():
        late_cols = slice(n_early * width, n_groups * width)
        project_rows(width, x_ref[...], dy_ref[...], weights[0, :, late_cols], weights[1, :, late_cols], weights[2, :, late_cols],
                     weights[3, late_cols, :], zout.at[p % 2], totals.at[1])
        put_z(p).start()

    t = jnp.where(step < base, step - FIRST, step - n_chunks)
    is_attention = ((step >= FIRST) & (step < FIRST + n_chunks)) | ((step >= base) & (step < n_chunks + att_steps))

    @pl.when((step == FIRST - 1) | (is_attention & (t < att_steps - 1)))
    def _():
        get_z(t + 1, lambda copy: copy.start())

    @pl.when((is_attention & (t >= 2)) | (step == n_chunks + att_steps) | (step == n_chunks + att_steps + 1))
    def _():
        put_stage(t - 2).wait()

    @pl.when(is_attention)
    def _():
        g = t // n_chunks

        @pl.when(t % n_chunks == 0)
        def _():
            state[...] = x_init[g // n_early, :, pl.ds((g % n_early) * per_group, per_group)]

        get_z(t, lambda copy: copy.wait())
        slot = t % 2
        row_id = lax.broadcasted_iota(jnp.int32, (BLOCK_LEN, BLOCK_LEN), 0)
        col_id = lax.broadcasted_iota(jnp.int32, (BLOCK_LEN, BLOCK_LEN), 1)
        causal = row_id >= col_id
        n_blocks = chunk // BLOCK_LEN
        pairs = [(h, b) for h in range(per_group) for b in range(n_blocks)]

        def block(i, h, b):
            start = i * width + h * HEAD_DIM
            return zin[slot, b * BLOCK_LEN:(b + 1) * BLOCK_LEN, start:start + HEAD_DIM]

        def beside(left, right):
            return jnp.concatenate([left, right], axis=1)

        def above(top, bottom):
            return jnp.concatenate([top, bottom], axis=0)

        for n, (h, b) in enumerate(pairs):
            q, k, v, do = (block(i, h, b) for i in range(4))
            k_t = k.T
            s16 = state[0, h].astype(BF16)
            state[0, h] += dot(k_t, v)
            r_run = state[1, h] - dot_tn(q, do)
            state[1, h] = r_run
            r16 = r_run.astype(BF16)
            mats[n, 0], mats[n, 1], mats[n, 2], mats[n, 3] = s16, s16.T, r16, r16.T
            a = jnp.where(causal, dot(q, k_t), 0.0).astype(BF16)
            e = jnp.where(causal, dot_nt(do, v), 0.0).astype(BF16)
            mats[n, 4], mats[n, 5], mats[n, 6], mats[n, 7] = a, a.T, e, e.T
        for n, (h, b) in enumerate(pairs):
            q, k, v, do = (block(i, h, b) for i in range(4))
            s16, s16_t, r16, r16_t, a, a_t, e, e_t = (mats[n, i] for i in range(8))
            values = (dot(beside(e, do), above(k, s16_t)), dot(beside(e_t, v), above(q, r16_t)),
                      dot(beside(a_t, k), above(do, r16)), dot(beside(a, q), above(v, s16)))
            for i, value in enumerate(values):
                start = i * width + h * HEAD_DIM
                stage[slot, b * BLOCK_LEN:(b + 1) * BLOCK_LEN, start:start + HEAD_DIM] = (att_scale * value).astype(BF16)
        put_stage(t).start()
        qkv = 3 * width

        @pl.when(t % n_chunks == 0)
        def _():
            part[g, :, :qkv] = dot_tn(x_ref[...], stage[slot, :, :qkv])
            part[g, :, qkv:] = dot_tn(dy_ref[...], stage[slot, :, qkv:])

        @pl.when(t % n_chunks > 0)
        def _():
            part[g, :, :qkv] += dot_tn(x_ref[...], stage[slot, :, :qkv])
            part[g, :, qkv:] += dot_tn(dy_ref[...], stage[slot, :, qkv:])

    tile = step - n_chunks - att_steps - 2

    @pl.when(tile == -1)
    def _():
        get_tile(0, lambda copy: copy.start())

    @pl.when((tile >= 0) & (tile < n_tiles))
    def _():
        @pl.when(tile + 1 < n_tiles)
        def _():
            get_tile(tile + 1, lambda copy: copy.start())

        get_tile(tile, lambda copy: copy.wait())

        def gather(i):
            return jnp.concatenate([zout[(tile % 2,) + tile_of(g) + (slice(i * width, (i + 1) * width),)] for g in range(n_groups)], axis=1)

        dx_ref[...] = (dot_nt(gather(0), weights[0]) + dot_nt(gather(1), weights[1]) + dot_nt(gather(2), weights[2])).astype(BF16)
        y_ref[...] = dot(gather(3), weights[3]).astype(BF16)


def assemble_kernel(n_groups, y_in, dx_in, grad_ref, y_ref, dx_ref, wq_ref, wk_ref, wv_ref, wo_ref):
    y_ref[...] = y_in[...]
    dx_ref[...] = dx_in[...]
    width = grad_ref.shape[2] // 4
    for g in range(n_groups):
        cols = slice(g * width, (g + 1) * width)
        for i, out in enumerate((wq_ref, wk_ref, wv_ref)):
            out[:, cols] = grad_ref[g, :, i * width:(i + 1) * width]
        wo_ref[cols, :] = grad_ref[g, :, 3 * width:].T


def solution(mesh):
    n_seq = mesh.shape["sp"]
    row_spec = P(("dp", "sp"), None)
    grad_spec = P("dp", None)

    def local_layer(tokens, w_q, w_k, w_v, w_o, grad_y):
        n_rows, dim = tokens.shape
        n_heads = dim // HEAD_DIM
        att_scale = 1.0 / math.sqrt(n_rows * n_seq * HEAD_DIM)
        tile = 512
        n_chips = n_seq // 2
        width, chunk, tile_rows = 2 * HEAD_DIM, n_rows // CHUNKS, TILE
        n_groups, n_tiles = dim // width, n_rows // TILE
        n_early = n_groups // 2
        early_cols = n_early * width
        rows_bf16 = jax.ShapeDtypeStruct((n_rows, dim), BF16)
        row_tile = pl.BlockSpec((tile, dim), lambda i: (i, 0))
        some_cols = pl.BlockSpec((dim, early_cols), lambda i: (0, 0), pipeline_mode=pl.Buffered(1))
        some_rows = pl.BlockSpec((early_cols, dim), lambda i: (0, 0), pipeline_mode=pl.Buffered(1))
        state_shape = (2, n_heads // 2, HEAD_DIM, HEAD_DIM)
        whole_state = pl.BlockSpec(state_shape, lambda i: (0, 0, 0, 0))
        half_rows = jax.ShapeDtypeStruct((n_early, n_rows, 4 * width), BF16)
        early, totals = pl.pallas_call(
            functools.partial(project_kernel, width),
            grid=(n_rows // tile,),
            in_specs=[row_tile, row_tile] + [some_cols] * 3 + [some_rows],
            out_specs=[pl.BlockSpec((n_early, tile, 4 * width), lambda i: (0, i, 0)), whole_state],
            out_shape=[half_rows, jax.ShapeDtypeStruct(state_shape, F32)],
            compiler_params=pltpu.CompilerParams(vmem_limit_bytes=VMEM_LIMIT, dimension_semantics=("arbitrary",)),
            name="project",
        )(tokens, grad_y, w_q, w_k, w_v, w_o)

        att_steps = n_groups * CHUNKS
        n_steps = CHUNKS + max(att_steps + 2 + n_tiles, att_steps + AT[6] + 1)

        def tile_index(s):
            return (jnp.clip(s - CHUNKS - att_steps - 2, 0, n_tiles - 1), 0)

        def chunk_index(s):
            late = jnp.minimum(s, CHUNKS + att_steps - 1) % CHUNKS
            return (jnp.where((s >= FIRST) & (s < FIRST + CHUNKS), s - FIRST, late), 0)

        row_chunk = pl.BlockSpec((chunk, dim), chunk_index)
        hbm = pl.BlockSpec(memory_space=pl.ANY)
        out_tile = pl.BlockSpec((tile_rows, dim), tile_index)
        chip_rows = dim // 2 // n_chips
        n_kinds = 13
        head_shape = (n_heads // 4, HEAD_DIM, HEAD_DIM)
        out_y, grad_x, grads, _, _ = pl.pallas_call(
            functools.partial(layer_kernel, att_scale, n_chips, n_groups, width),
            grid=(n_steps,),
            in_specs=[row_chunk] * 2 + [whole_state] + [hbm] * 5,
            out_specs=[out_tile] * 2 + [hbm] * 3,
            out_shape=[rows_bf16] * 2 + [jax.ShapeDtypeStruct((n_groups, dim, 4 * width), F32),
                                         jax.ShapeDtypeStruct((n_groups, n_rows, 4 * width), BF16), half_rows],
            scratch_shapes=[
                pltpu.VMEM((2, width // HEAD_DIM, HEAD_DIM, HEAD_DIM), F32),
                pltpu.VMEM((2, chunk, 4 * width), BF16),
                pltpu.VMEM((n_groups, dim, 4 * width), F32),
                pltpu.VMEM((2, dim // 2, 4 * width), F32),
                pltpu.VMEM((2, 2, chip_rows // 2, 4 * width), F32),
                pltpu.VMEM((2, 2, chip_rows, 4 * width), F32),
                pltpu.VMEM((4, dim, dim), BF16),
                pltpu.VMEM((2, chunk, 4 * width), BF16),
                pltpu.VMEM((2, n_early, chunk, 4 * width), BF16),
                pltpu.VMEM((width // HEAD_DIM * (chunk // BLOCK_LEN), 8, BLOCK_LEN, HEAD_DIM), BF16),
                pltpu.VMEM((2,) + state_shape, F32),
                pltpu.VMEM((2,) + state_shape, F32),
                pltpu.VMEM((2, 2) + head_shape, F32),
                pltpu.VMEM((2, n_chips - 1) + head_shape, F32),
                pltpu.VMEM((2, 2, 2) + head_shape, F32),
                pltpu.VMEM((2,) + state_shape, F32),
                pltpu.SemaphoreType.DMA((2,)),
                pltpu.SemaphoreType.DMA((4,)),
                pltpu.SemaphoreType.DMA((2, n_groups)),
                pltpu.SemaphoreType.DMA((n_groups,)),
                pltpu.SemaphoreType.DMA((n_kinds, n_groups)),
                pltpu.SemaphoreType.DMA((n_kinds, n_groups)),
                pltpu.SemaphoreType.DMA((2,)),
                pltpu.SemaphoreType.DMA((2,)),
                pltpu.SemaphoreType.DMA((n_chips + 1, 2)),
                pltpu.SemaphoreType.DMA((n_chips + 1, 2)),
            ],
            compiler_params=pltpu.CompilerParams(vmem_limit_bytes=VMEM_LIMIT, dimension_semantics=("arbitrary",), collective_id=1, has_side_effects=True),
            name="layer",
        )(tokens, grad_y, totals, early, w_q, w_k, w_v, w_o)

        slab = 128
        n_slabs = dim // slab
        out_rows = pl.BlockSpec((n_rows // n_slabs, dim), lambda i: (i, 0))
        return pl.pallas_call(
            functools.partial(assemble_kernel, n_groups),
            grid=(n_slabs,),
            in_specs=[out_rows] * 2 + [pl.BlockSpec((n_groups, slab, 4 * width), lambda i: (0, i, 0))],
            out_specs=[out_rows] * 2 + [pl.BlockSpec((slab, dim), lambda i: (i, 0))] * 3 + [pl.BlockSpec((dim, slab), lambda i: (0, i))],
            out_shape=[rows_bf16] * 2 + [jax.ShapeDtypeStruct((dim, dim), F32)] * 4,
            compiler_params=pltpu.CompilerParams(vmem_limit_bytes=VMEM_LIMIT, dimension_semantics=("arbitrary",)),
            name="assemble",
        )(out_y, grad_x, grads)

    return jax.shard_map(local_layer, mesh=mesh, in_specs=(row_spec, P(), P(), P(), P(), row_spec),
                         out_specs=(row_spec, row_spec) + (grad_spec,) * 4, check_vma=False)
```
